32 devices in a mesh: blk: 8 (over z, x), dp: 4 (over y, core).
Axes of the slice: x: 2, y: 2, z: 4, core: 2. Of those that a mesh axis runs over, the one named last changes fastest.
Arguments:
- tokens: bfloat16 [1024, 5120], P('blk', 'dp'), may hold values from -6 to 6
- expert_ids: int32 [1024, 6], P('blk'), may hold values from 0 to 15, all different within a row; in each aligned block of 128 rows (0 to 127, 128 to 255, ...) at most 96 rows name the same one
- gate_vals: float32 [1024, 6], P('blk'), may hold values from 0.1 to 1
- w_gate: bfloat16 [16, 5120, 1536], P('blk', 'dp'), may hold values from -0.078125 to 0.078125
- w_up: bfloat16 [16, 5120, 1536], P('blk', 'dp'), may hold values from -0.078125 to 0.078125
- w_down: bfloat16 [16, 5120, 1536], P('blk', 'dp'), may hold values from -0.15625 to 0.15625
Outputs:
- combined: bfloat16 [1024, 5120], P('blk', 'dp')
The draws below stay inside these ranges and needn't reach their ends.
Inputs may be any that keep to these rules, and one draw needn't show every extreme that they name: `expert_ids`: each row names 6 different experts. Among the 128 rows of one index of blk (aligned blocks) no expert is named more than 96 times, a bound that some block reaches.
All inputs are finite; a program needn't handle non-finite values.
Results may differ from the reference program's by a relative error of at most 0.0057.
Values may be sent and summed in bfloat16 or wider, within the bound.
No kernel may reach another device: no remote copies, remote signals or barrier semaphores. Data moves between devices by JAX's collectives and lax.ppermute only.
A program may use at most 128 MiB of HBM per device.

```python
import math
import jax
import jax.numpy as jnp
import numpy as np
from jax import lax

D = 5120
FF = 1536
TOP = 6
TOK_DEV = 128
EXPERTS = 16
TOKENS = 1024
CAP = 96
N_BLK = 8


def levels(rng, shape, shards, low, top_value):
    factor_of = 1.0
    for dim, parts in shards:
        steps = jax.random.uniform(jax.random.fold_in(jax.random.fold_in(rng, 6), dim), (parts,), jnp.float32, low / len(shards), top_value / len(shards))
        factor_of = factor_of * jnp.repeat(jnp.exp(steps), shape[dim] // parts).reshape((-1,) + (1,) * (len(shape) - 1 - dim))
    return factor_of


def deal_out(rng, own, number, rows, count, top, bound, slope):
    ranking = jax.random.permutation(rng, count)
    packed, ordinary = load_shares(count, rows * top, bound, slope, True), load_shares(count, rows * top, bound, slope, False)
    places = jnp.arange(count)

    def named(tallies, turn):
        used = int((tallies > 0).sum())
        fixed = max(1, used // 4)
        moved = fixed + (places - fixed + turn * (used - fixed)) % max(1, count - fixed)
        return jnp.zeros((count,), jnp.int32).at[ranking[jnp.where(places < fixed, places, moved)]].set(jnp.asarray(tallies, jnp.int32))

    tallies = jnp.where(number % 4 == 0, named(packed, number // 4), named(ordinary, number - number // 4 - 1))
    mixed = jax.random.permutation(jax.random.fold_in(own, 3), count)
    source_of, taker = mixed[0:count // 2 * 2:2], mixed[1:count // 2 * 2:2]
    room = jnp.minimum(tallies[source_of] - 1, bound - tallies[taker]) // 2
    room = jnp.where((source_of == ranking[0]) | (taker == ranking[0]) | (tallies[taker] == 0), 0, jnp.maximum(room, 0))
    moved = jax.random.randint(jax.random.fold_in(own, 4), (count // 2,), 0, 1 << 20) % (room + 1)
    tallies = tallies.at[source_of].add(-moved).at[taker].add(moved)
    items = jnp.searchsorted(jnp.cumsum(tallies), jnp.arange(rows * top), side="right").astype(jnp.int32)
    grid = items.reshape(top, rows).T
    grid = grid[jax.random.permutation(jax.random.fold_in(own, 1), rows)]
    turn = jax.random.randint(jax.random.fold_in(own, 2), (rows, 1), 0, top)
    return jnp.take_along_axis(grid, (jnp.arange(top)[None, :] + turn) % top, axis=1)


def load_shares(amount, total, most, slope, full):
    loads = [(1 << 20) // math.isqrt(rank ** slope) + 1 for rank in range(1, amount + 1)]
    largest = most if full else min(most, max(-(-total // amount), total * loads[0] // sum(loads)))
    least = 1 if total - largest >= amount - 1 else 0
    counts, spare = [largest] + [least] * (amount - 1), total - largest - least * (amount - 1)
    while spare > 0:
        free = [i for i in range(1, amount) if counts[i] < largest] or [i for i in range(1, amount) if counts[i] < most]
        pool, remaining = sum([loads[i] for i in free]), spare
        for i in free:
            more = min(most - counts[i], max(1, remaining * loads[i] // pool), spare)
            counts[i] = counts[i] + more
            spare = spare - more
    return np.array(counts)


def gaussian(key, extent, deviation, most, split=(), held_as=jnp.bfloat16):
    array = jax.random.normal(key, extent, jnp.float32) * deviation
    if len(split) > 0:
        array = levels(key, extent, split, -0.22, 0.18) * array
    return jnp.clip(array, min=-most, max=most).astype(held_as)


def setup_inputs(seed: int = 0) -> dict:
    streams_of = jax.random.split(jax.random.key(seed), 7)
    tokens = gaussian(streams_of[0], (TOKENS, D), 1.0, 6.0, ((0, 8), (1, 4)))
    expert_ids_keys = jax.random.split(jax.random.fold_in(streams_of[1], 1), TOKENS // TOK_DEV)
    expert_ids_turns = jax.random.permutation(jax.random.fold_in(streams_of[1], 3), TOKENS // TOK_DEV)
    expert_ids = jax.vmap(lambda own, number: deal_out(jax.random.fold_in(streams_of[1], 2), own, number, TOK_DEV, EXPERTS, TOP, CAP, 2))(expert_ids_keys, expert_ids_turns).reshape((TOKENS, TOP))
    gate_vals = jnp.clip(jnp.exp(math.log(1.0) - 2.3025851 * jax.random.uniform(streams_of[2], (TOKENS, TOP), jnp.float32) ** levels(streams_of[2], (TOKENS, TOP), ((0, 8),), -0.2, 0.2)), 0.1, 1.0)
    w_gate = gaussian(streams_of[3], (EXPERTS, D, FF), D ** -0.5, 0.078125, ((0, 8), (1, 4)))
    w_up = gaussian(streams_of[4], (EXPERTS, D, FF), D ** -0.5, 0.078125, ((0, 8), (1, 4)))
    w_down = gaussian(streams_of[5], (EXPERTS, D, FF), FF ** -0.5, 0.15625, ((0, 8), (1, 4)))
    return dict(tokens=tokens, expert_ids=expert_ids, gate_vals=gate_vals, w_gate=w_gate, w_up=w_up, w_down=w_down)


def reference(tokens, expert_ids, gate_vals, w_gate, w_up, w_down):
    rows_all = N_BLK * CAP
    pairs = expert_ids.reshape(N_BLK, TOK_DEV * TOP)
    onehot = (pairs[:, :, None] == jnp.arange(EXPERTS, dtype=jnp.int32)[None, None, :]).astype(jnp.int32)
    before = jnp.cumsum(onehot, axis=1) - onehot
    position = jnp.sum(before * onehot, axis=2).astype(jnp.int32)
    source = jnp.arange(N_BLK, dtype=jnp.int32)[:, None]
    slot_index = (pairs * rows_all + source * CAP + position).reshape(-1).astype(jnp.int32)
    copies = jnp.repeat(tokens, TOP, axis=0)
    buffer = jnp.zeros((EXPERTS * rows_all, D), tokens.dtype).at[slot_index].set(copies)
    buffer = buffer.reshape(EXPERTS, rows_all, D)

    def expert_fn(items):
        row_block, gate_w, up_w, down_w = items
        gate_part = jnp.dot(row_block, gate_w, preferred_element_type=jnp.float32)
        up_part = jnp.dot(row_block, up_w, preferred_element_type=jnp.float32)
        hidden = (jax.nn.silu(gate_part) * up_part).astype(jnp.bfloat16)
        output = lax.dot_general(hidden, down_w, (((1,), (1,)), ((), ())), preferred_element_type=jnp.float32)
        return output.astype(jnp.bfloat16)

    outputs = lax.map(expert_fn, (buffer, w_gate, w_up, w_down)).reshape(EXPERTS * rows_all, D)
    picked = outputs[slot_index].astype(jnp.float32).reshape(TOKENS, TOP, D)
    combined = jnp.sum(picked * gate_vals[:, :, None], axis=1)
    return combined.astype(jnp.bfloat16)
```

```python
import functools

import jax
import jax.numpy as jnp
from jax import lax
from jax.experimental import pallas as pl
from jax.experimental.pallas import tpu as pltpu
from jax.sharding import PartitionSpec as P

INFO = 128
F32 = jnp.float32
BF16 = jnp.bfloat16


def params(mib):
    return pltpu.CompilerParams(vmem_limit_bytes=mib * 2**20)


def pack_kernel(tok_ref, ids_ref, gate_ref, out_ref):
    rows, width = tok_ref.shape
    top_k = ids_ref.shape[1]
    count = INFO // 4
    lane = lax.broadcasted_iota(jnp.int32, (rows, INFO), 1)
    expert = lane % count
    group = lane // count
    named = jnp.zeros((rows, INFO), F32)
    gate = jnp.zeros((rows, INFO), F32)
    for k in range(top_k):
        hit = ids_ref[:, k : k + 1] == expert
        named = jnp.where(hit, 1.0, named)
        gate = jnp.where(hit, gate_ref[:, k : k + 1], gate)
    earlier = lax.broadcasted_iota(jnp.int32, (rows, rows), 1) < lax.broadcasted_iota(
        jnp.int32, (rows, rows), 0
    )
    rank = jnp.dot(earlier.astype(BF16), named.astype(BF16), preferred_element_type=F32)
    slot = jnp.where(named > 0, rank, float(rows))
    first = gate.astype(BF16).astype(F32)
    second = (gate - first).astype(BF16).astype(F32)
    third = gate - first - second
    info = jnp.where(
        group == 0, slot, jnp.where(group == 1, first, jnp.where(group == 2, second, third))
    )
    out_ref[:, :width] = tok_ref[...]
    out_ref[:, width:] = info.astype(BF16)


def up_kernel(blocks, cap, pick_ref, rows_ref, *refs):
    packed = refs[:blocks]
    gate_ref, up_ref, out_ref, x_ref = refs[blocks:]
    width = gate_ref.shape[1]
    column = pick_ref[1]

    @pl.when(pl.program_id(0) == 0)
    def _():
        total = None
        for i in range(blocks):
            info = packed[i][:, width:].astype(F32).T
            line = lax.broadcasted_iota(jnp.int32, info.shape, 0) == column
            slot = jnp.sum(jnp.where(line, info, 0.0), axis=0, keepdims=True)
            hit = (rows_ref[...] - i * cap) == slot.astype(jnp.int32)
            hit = hit & (rows_ref[...] >= i * cap) & (rows_ref[...] < (i + 1) * cap)
            part = jnp.dot(
                hit.astype(F32).astype(BF16), packed[i][:, :width], preferred_element_type=F32
            )
            total = part if total is None else total + part
        x_ref[...] = total.astype(BF16)

    x = x_ref[...]
    out_ref[0] = jnp.dot(x, gate_ref[0], preferred_element_type=F32).astype(out_ref.dtype)
    out_ref[1] = jnp.dot(x, up_ref[0], preferred_element_type=F32).astype(out_ref.dtype)


def up_call(packed, pick, rows, w_gate, w_up, cap, dtype):
    blocks = len(packed)
    tok_rows = packed[0].shape[0]
    width, hidden = w_gate.shape[1:]
    count = blocks * cap
    tile = 256 if hidden % 256 == 0 else hidden
    weight = pl.BlockSpec((1, width, tile), lambda j, pick: (pick[0], 0, j))
    whole = lambda shape: pl.BlockSpec(shape, lambda j, pick: (0,) * len(shape))
    return pl.pallas_call(
        functools.partial(up_kernel, blocks, cap),
        grid_spec=pltpu.PrefetchScalarGridSpec(
            num_scalar_prefetch=1,
            grid=(hidden // tile,),
            in_specs=[whole((count, 1))]
            + [whole((tok_rows, width + INFO))] * blocks
            + [weight, weight],
            out_specs=pl.BlockSpec((2, count, tile), lambda j, pick: (0, 0, j)),
            scratch_shapes=[pltpu.VMEM((count, width), BF16)],
        ),
        out_shape=jax.ShapeDtypeStruct((2, count, hidden), dtype),
        compiler_params=params(20),
        cost_estimate=pl.CostEstimate(
            flops=4 * max(count, 256) * width * hidden,
            bytes_accessed=4 * width * hidden,
            transcendentals=0,
        ),
    )(pick, rows, *packed, w_gate, w_up)


def down_kernel(blocks, cap, pick_ref, rows_ref, *refs):
    packed = refs[:blocks]
    hidden = refs[blocks : blocks + 2]
    down_ref = refs[blocks + 2]
    outs = refs[blocks + 3 : 2 * blocks + 3]
    place_ref, gate_ref = refs[2 * blocks + 3 :]
    width = packed[0].shape[1] - INFO
    experts = INFO // 4

    @pl.when(pl.program_id(0) == 0)
    def _():
        for i in range(blocks):
            info = packed[i][:, width:].astype(F32)
            lane = lax.broadcasted_iota(jnp.int32, info.shape, 1)
            for e in range(2):
                column = pick_ref[e, 1]
                take = lambda mask: jnp.sum(jnp.where(mask, info, 0.0), axis=1, keepdims=True)
                slot = take(lane == column).astype(jnp.int32)
                own = (rows_ref[...] >= i * cap) & (rows_ref[...] < (i + 1) * cap)
                hit = ((rows_ref[...] - i * cap) == slot) & own
                place_ref[e, i] = hit.astype(F32).astype(BF16)
                value = take((lane % experts == column) & (lane >= experts))
                gate_ref[e, i] = jnp.broadcast_to(value, gate_ref.shape[2:])

    totals = [None] * blocks
    for e in range(2):
        full = lax.dot_general(
            hidden[e][...],
            down_ref[pick_ref[e, 0]],
            (((1,), (1,)), ((), ())),
            preferred_element_type=F32,
        ).astype(BF16)
        for i in range(blocks):
            rows = jnp.dot(place_ref[e, i], full, preferred_element_type=F32)
            term = rows * gate_ref[e, i][:, :1]
            totals[i] = term if totals[i] is None else totals[i] + term
    for i in range(blocks):
        outs[i][...] = totals[i].astype(outs[i].dtype)


def down_call(packed, pick, rows, hidden, w_down, cap, dtypes):
    blocks = len(packed)
    tok_rows = packed[0].shape[0]
    width, ff = w_down.shape[1:]
    count = blocks * cap
    tile = 256 if width % 256 == 0 else width
    whole = lambda shape: pl.BlockSpec(shape, lambda j, pick: (0,) * len(shape))
    return pl.pallas_call(
        functools.partial(down_kernel, blocks, cap),
        grid_spec=pltpu.PrefetchScalarGridSpec(
            num_scalar_prefetch=1,
            grid=(width // tile,),
            in_specs=[whole((1, count))]
            + [whole((tok_rows, width + INFO))] * blocks
            + [whole((count, ff))] * 2
            + [pl.BlockSpec((2, tile, ff), lambda j, pick: (0, j, 0))],
            out_specs=[pl.BlockSpec((tok_rows, tile), lambda j, pick: (0, j))] * blocks,
            scratch_shapes=[
                pltpu.VMEM((2, blocks, tok_rows, count), BF16),
                pltpu.VMEM((2, blocks, tok_rows, 128), F32),
            ],
        ),
        out_shape=[jax.ShapeDtypeStruct((tok_rows, width), d) for d in dtypes],
        compiler_params=params(20),
        cost_estimate=pl.CostEstimate(
            flops=4 * max(count, 256) * width * ff,
            bytes_accessed=4 * width * ff,
            transcendentals=0,
        ),
    )(pick, rows, *packed, *hidden, w_down)


def local(tokens, expert_ids, gate_vals, w_gate, w_up, w_down):
    n_blk = lax.axis_size("blk")
    n_dp = lax.axis_size("dp")
    tok_rows, width = tokens.shape
    top_k = expert_ids.shape[1]
    held, _, ff = w_gate.shape
    cap = 2 * tok_rows * top_k // (held * n_blk)
    assert held == 2 and n_dp % 2 == 0 and n_blk % 2 == 0
    blk = lax.axis_index("blk")
    dp = lax.axis_index("dp")
    core, group = dp % 2, dp // 2
    units = n_dp // 2
    ring = n_blk // 2

    def flip(x, bit):
        return lax.ppermute(x, "dp", [(i, i ^ bit) for i in range(n_dp)])

    def across(x):
        return lax.ppermute(x, "blk", [(i, i ^ 1) for i in range(n_blk)])

    def along(x, steps):
        return lax.ppermute(x, "blk", [(i, (i + 2 * steps) % n_blk) for i in range(n_blk)])

    own = pl.pallas_call(
        pack_kernel,
        out_shape=jax.ShapeDtypeStruct((tok_rows, width + INFO), BF16),
        cost_estimate=pl.CostEstimate(flops=10**8, bytes_accessed=10**6, transcendentals=0),
    )(tokens, expert_ids, gate_vals)
    held_tokens = {(0, 0): own}
    for s in range(ring):
        if s > 0:
            held_tokens[s, 0] = along(held_tokens[s - 1, 0], 1)
        held_tokens[s, 1] = across(held_tokens[s, 0])

    mine = jnp.stack([core, held * blk + core]).astype(jnp.int32)
    other = jnp.stack([1 - core, held * blk + 1 - core]).astype(jnp.int32)
    both = jnp.stack([mine, other])

    chunks = [[(0, 0)], [(1, 0)]]
    chunks += [[(s, 1), (s + 1, 0)] for s in range(1, ring - 1)]
    chunks += [[(ring - 1, 1)], [(0, 1)]]
    given = {}
    for chunk in chunks:
        packed = [held_tokens[b] for b in chunk]
        count = len(chunk) * cap
        unit = count // units
        position = jnp.arange(count, dtype=jnp.int32)
        rows = ((position // unit) ^ group) * unit + position % unit
        column, line = rows[:, None], rows[None, :]
        sent = up_call(packed, other, column, w_gate, w_up, cap, BF16)
        arrived = flip(sent, 1)
        kept = up_call(packed, mine, column, w_gate, w_up, cap, F32)
        bits = [2 << i for i in range(units.bit_length() - 1)]
        kept = kept + arrived.astype(F32)
        for bit in reversed(bits):
            half = kept.shape[1] // 2
            arrived = flip(kept[:, half:].astype(BF16), bit)
            kept = kept[:, :half] + arrived.astype(F32)
        hidden = (jax.nn.silu(kept[0]) * kept[1]).astype(BF16)
        for bit in bits:
            hidden = jnp.concatenate([hidden, flip(hidden, bit)], axis=0)
        hidden = (hidden, flip(hidden, 1))
        dtypes = [BF16 if b[1] else F32 for b in chunk]
        given.update(zip(chunk, down_call(packed, both, line, hidden, w_down, cap, dtypes)))

    total = None
    for s in range(ring):
        part = given[s, 0] + across(given[s, 1]).astype(F32)
        if s > 0:
            part = along(part.astype(BF16), -s).astype(F32)
        total = part if total is None else total + part
    return total.astype(BF16)


def solution(mesh):
    return jax.shard_map(
        local,
        mesh=mesh,
        in_specs=(
            P("blk", "dp"),
            P("blk", None),
            P("blk", None),
            P("blk", "dp", None),
            P("blk", "dp", None),
            P("blk", "dp", None),
        ),
        out_specs=P("blk", "dp"),
        check_vma=False,
    )
```
